32 devices in a mesh: fsdp: 8 (over z, y), seq: 4 (over x, core).
Axes of the slice: x: 2, y: 2, z: 4, core: 2. Of those that a mesh axis runs over, the one named last changes fastest.
Arguments:
- tokens: bfloat16 [8, 512, 4096], P('fsdp'), may hold values from -7 to 7
- norm_gain: float32 [4096], replicated, may hold values from 0.1 to 1.9
- curvature: bfloat16 [8, 512, 4096], P('fsdp'), may hold values from 0.19921875 to 2
- weight_slots: bfloat16 [4, 400, 128, 128], P('seq', 'fsdp'), may hold values from -1 to 1
- probe_slots: bfloat16 [4, 400, 128, 128], P('seq', 'fsdp'), may hold values from -0.09375 to 0.09375
- block_counts: int32 [4, 8], P('seq'), may hold values from 1 to 50, 320 in all within a row
Outputs:
- hvp_slots: float32 [4, 400, 128, 128], P('seq', 'fsdp')
The draws below stay inside these ranges and needn't reach their ends.
Inputs may be any that keep to these rules, and one draw needn't show every extreme that they name: `block_counts`: in each row, device d along fsdp owns the n_d blocks that follow the earlier devices' blocks, in its first n_d slots; a row sums to 320, and 50 is reached in every row.
All inputs are finite; a program needn't handle non-finite values.
Results may differ from the reference program's by a relative error of at most 0.018.
Values may be sent and summed in bfloat16 or wider, within the bound.
No kernel may reach another device: no remote copies, remote signals or barrier semaphores. Data moves between devices by JAX's collectives and lax.ppermute only.
A program may use at most 128 MiB of HBM per device.

```python
import math
import jax
import jax.numpy as jnp
import numpy as np
from jax import lax

D = 4096
HQ = 16
HK = 4
HD = 128
BLK = 128
LEN = 512
NB = 320
SLOTS = 50
N_FSDP = 8
N_SEQ = 4


def draw_tokens(key, part):
    own_key = jax.random.fold_in(key, 11)
    noise = jax.random.normal(own_key, (N_FSDP, LEN, D), jnp.float32)
    result = jnp.clip(noise, -6.0, 6.0)
    return result.astype(jnp.bfloat16)


def draw_weight_slots(key, part):
    own_key = jax.random.fold_in(key, 12)
    result = jnp.clip(jax.random.normal(own_key, (N_SEQ, N_FSDP * SLOTS, BLK, BLK), jnp.float32), -6.0, 6.0) * D ** (-0.5)
    return result.astype(jnp.bfloat16)


def block_scale(key, extent, shards, least, largest):
    def one(axis_at, blocks):
        heights = jax.random.uniform(jax.random.fold_in(jax.random.fold_in(key, 6), axis_at), (blocks,), jnp.float32, least / len(shards), largest / len(shards))
        return jnp.repeat(jnp.exp(heights), extent[axis_at] // blocks).reshape((-1,) + (1,) * (len(extent) - axis_at - 1))

    gain = one(*shards[0])
    for cut in shards[1:]:
        gain = gain * one(*cut)
    return gain


def length_profile(number_of, total, reach, skew):
    weights = [(1 << 20) // math.isqrt(grade ** skew) + 1 for grade in range(2, number_of + 1)]
    surplus, holding = total - reach - (number_of - 1), [1] * (number_of - 1)
    while surplus > 0:
        candidates = [i for i in range(number_of - 1) if holding[i] < reach]
        whole, left = sum([weights[i] for i in candidates]), surplus
        for i in candidates:
            more = min(reach - holding[i], max(1, left * weights[i] // whole), surplus)
            holding[i] = holding[i] + more
            surplus = surplus - more
    return np.array([reach] + holding)


def ragged_sizes(key, count, total, bound, slope):
    if count == 2:
        one = jax.random.randint(key, (), max(1, total - bound), min(bound, total - 1) + 1)
        return jnp.stack([one, total - one])
    lengths = jnp.asarray(length_profile(count, total, bound, slope), jnp.int32)
    couples = (count - 1) // 2
    giver, receiver = lengths[1:1 + 2 * couples:2], lengths[2:2 + 2 * couples:2]
    margin = jnp.minimum(giver - 1, bound - receiver)
    moved = jax.random.randint(jax.random.fold_in(key, 1), (couples,), 0, 1 << 20) % (margin + 1)
    lengths = lengths.at[1:1 + 2 * couples:2].set(giver - moved).at[2:2 + 2 * couples:2].set(receiver + moved)
    return lengths[jax.random.permutation(jax.random.fold_in(key, 2), count)]


def centred(rng, dims, deviation, bound, cuts=(), kind=jnp.bfloat16):
    loudness = block_scale(rng, dims, cuts, -0.22, 0.18) if cuts else 1.0
    values = jax.random.normal(rng, dims, jnp.float32) * deviation * loudness
    return jnp.minimum(jnp.maximum(values, -bound), bound).astype(kind)


def setup_inputs(seed: int = 0) -> dict:
    streams_of = jax.random.split(jax.random.key(seed), 7)
    tokens = draw_tokens(jax.random.fold_in(streams_of[6], 71), 0)
    norm_gain = jnp.clip(1.0 + 0.18 * jax.random.normal(streams_of[1], (D,), jnp.float32), 0.1, 1.9)
    curvature = jnp.clip(jnp.exp(math.log(2.0) - 2.306499 * jax.random.uniform(streams_of[2], (N_FSDP, LEN, D), jnp.float32) ** block_scale(streams_of[2], (N_FSDP, LEN, D), ((0, 8),), -0.2, 0.2)), 0.19921875, 2.0).astype(jnp.bfloat16)
    weight_slots = draw_weight_slots(jax.random.fold_in(streams_of[6], 71), 0)
    probe_slots = centred(streams_of[4], (N_SEQ, N_FSDP * SLOTS, BLK, BLK), D ** -0.5, 0.09375, ((0, 4), (1, 8)))
    block_counts = jax.vmap(lambda own: ragged_sizes(own, N_FSDP, NB, SLOTS, 2))(jax.random.split(streams_of[5], N_SEQ)).reshape((N_SEQ, N_FSDP)).astype(jnp.int32)
    return dict(tokens=tokens, norm_gain=norm_gain, curvature=curvature, weight_slots=weight_slots, probe_slots=probe_slots, block_counts=block_counts)


THETA = 500000.0
EPS = 1e-05
NEGATIVE = -1e+30

def rotary(length, head_dim):
    half_dim = head_dim // 2
    frequency = jnp.exp(-jnp.log(THETA) * 2.0 * jnp.arange(half_dim, dtype=jnp.float32) / head_dim)
    angles = jnp.arange(length, dtype=jnp.float32)[:, None] * frequency[None, :]
    return (jnp.cos(angles)[:, None, :], jnp.sin(angles)[:, None, :])

def rotate(field_in, cosine, sine):
    half_dim = field_in.shape[-1] // 2
    first_half = field_in[..., :half_dim]
    second = field_in[..., half_dim:]
    return jnp.concatenate([first_half * cosine - second * sine, second * cosine + first_half * sine], axis=-1)

def normalize(tokens, norm_gain):
    values = tokens.astype(jnp.float32)
    factor = lax.rsqrt(lax.optimization_barrier(jnp.mean(values * values, axis=-1, keepdims=True)) + EPS)
    return (values * factor * norm_gain).astype(jnp.bfloat16)

def attention_branch(w_qkv, w_out, normed, cosine, sine, q_heads, kv_heads):
    length = normed.shape[0]
    head_dim = w_out.shape[0] // q_heads
    projected = jnp.dot(normed, w_qkv, preferred_element_type=jnp.float32)
    q_end = q_heads * head_dim
    k_end = q_end + kv_heads * head_dim
    queries = rotate(projected[:, :q_end].reshape(length, q_heads, head_dim), cosine, sine).astype(jnp.bfloat16)
    key_rows = rotate(projected[:, q_end:k_end].reshape(length, kv_heads, head_dim), cosine, sine).astype(jnp.bfloat16)
    values = projected[:, k_end:].reshape(length, kv_heads, head_dim).astype(jnp.bfloat16)
    queries, key_rows, values = lax.optimization_barrier((queries, key_rows, values))
    queries = queries.reshape(length, kv_heads, q_heads // kv_heads, head_dim)
    scores = jnp.einsum('qkgd,skd->kgqs', queries.astype(jnp.float32), key_rows.astype(jnp.float32)) * head_dim ** (-0.5)
    causal = jnp.arange(length)[:, None] >= jnp.arange(length)[None, :]
    scores = jnp.where(causal, scores, NEGATIVE)
    attn_probs = jax.nn.softmax(scores, axis=-1).astype(jnp.bfloat16)
    attn_probs = lax.optimization_barrier(attn_probs)
    mixed_heads = jnp.einsum('kgqs,skd->qkgd', attn_probs.astype(jnp.float32), values.astype(jnp.float32))
    mixed_heads = mixed_heads.reshape(length, q_heads * head_dim).astype(jnp.bfloat16)
    return jnp.dot(mixed_heads, w_out, preferred_element_type=jnp.float32)

def owner_slots(counts, blocks, slots):
    range_ends = jnp.cumsum(counts).astype(jnp.int32)
    starts = (range_ends - counts).astype(jnp.int32)
    block_ids = jnp.arange(blocks, dtype=jnp.int32)
    owners = lax.optimization_barrier(jnp.sum((range_ends[None, :] <= block_ids[:, None]).astype(jnp.int32), axis=1)).astype(jnp.int32)
    owner_hot = owners[:, None] == jnp.arange(counts.shape[0], dtype=jnp.int32)[None, :]
    first_block = lax.optimization_barrier(jnp.sum(jnp.where(owner_hot, starts[None, :], 0), axis=1)).astype(jnp.int32)
    return (owners * slots + block_ids - first_block).astype(jnp.int32)

def to_matrix(blocks, row_blocks, col_blocks):
    blk_edge = blocks.shape[-1]
    return blocks.reshape(row_blocks, col_blocks, blk_edge, blk_edge).transpose(0, 2, 1, 3).reshape(row_blocks * blk_edge, col_blocks * blk_edge)

def to_blocks(matrix, blk_edge):
    row_blocks = matrix.shape[0] // blk_edge
    col_blocks = matrix.shape[1] // blk_edge
    return matrix.reshape(row_blocks, blk_edge, col_blocks, blk_edge).transpose(0, 2, 1, 3).reshape(row_blocks * col_blocks, blk_edge, blk_edge)

def reference(tokens, norm_gain, curvature, weight_slots, probe_slots, block_counts):
    n_columns = weight_slots.shape[0]
    q_heads = HQ // n_columns
    kv_heads = HK // n_columns
    row_blocks = D // BLK
    qkv_cols = (q_heads + 2 * kv_heads) * HD // BLK
    out_rows = q_heads * HD // BLK
    qkv_split = row_blocks * qkv_cols
    cosine, sine = rotary(LEN, HD)
    normed = jax.vmap(normalize, in_axes=(0, None))(tokens, norm_gain)
    tangent_sum = jnp.zeros((N_FSDP, LEN, D), jnp.float32)
    unpacked = []
    for column in range(n_columns):
        slot_of = owner_slots(block_counts[column], NB, SLOTS)
        w_blocks = weight_slots[column][slot_of]
        p_blocks = probe_slots[column][slot_of]
        w_qkv = to_matrix(w_blocks[:qkv_split], row_blocks, qkv_cols)
        w_out = to_matrix(w_blocks[qkv_split:], out_rows, row_blocks)
        p_qkv = to_matrix(p_blocks[:qkv_split], row_blocks, qkv_cols)
        p_out = to_matrix(p_blocks[qkv_split:], out_rows, row_blocks)

        def tangent_one(seq_normed, w_qkv=w_qkv, w_out=w_out, p_qkv=p_qkv, p_out=p_out):

            def inner(first_w, second_w):
                return attention_branch(first_w, second_w, seq_normed, cosine, sine, q_heads, kv_heads)
            return jax.jvp(inner, (w_qkv, w_out), (p_qkv, p_out))[1]
        tangent_sum = tangent_sum + lax.map(tangent_one, normed)
        unpacked.append((slot_of, w_qkv, w_out))
    weighted = (curvature.astype(jnp.float32) * tangent_sum).astype(jnp.bfloat16)
    factor = 1.0 / jnp.sqrt(jnp.float32(LEN * N_FSDP))
    results = []
    for column in range(n_columns):
        slot_of, w_qkv, w_out = unpacked[column]

        def accumulate(grad_total, seq_pair, w_qkv=w_qkv, w_out=w_out):
            seq_normed, seq_weighted = seq_pair

            def inner(first_w, second_w):
                return attention_branch(first_w, second_w, seq_normed, cosine, sine, q_heads, kv_heads)
            _, pullback = jax.vjp(inner, w_qkv, w_out)
            g_qkv, g_out = pullback(seq_weighted.astype(jnp.float32))
            grad_blocks = jnp.concatenate([to_blocks(g_qkv, BLK), to_blocks(g_out, BLK)], axis=0)
            return (grad_total + grad_blocks.astype(jnp.float32), None)
        grad_total, _ = lax.scan(accumulate, jnp.zeros((NB, BLK, BLK), jnp.float32), (normed, weighted))
        packed = jnp.zeros((N_FSDP * SLOTS, BLK, BLK), jnp.float32).at[slot_of].set(grad_total * factor)
        results.append(packed)
    return jnp.stack(results)
```

```python
import jax
import jax.numpy as jnp
from jax import lax
from jax.experimental import pallas as pl
from jax.experimental.pallas import tpu as pltpu
from jax.sharding import PartitionSpec as P

D = 4096
HQ = 16
HK = 4
HD = 128
BLK = 128

THETA = 500000.0
EPS = 1e-05
NEGATIVE = -1e30

STREAMS = 4
F32 = jnp.float32
BF16 = jnp.bfloat16


def rotary(length, head_dim):
    half_dim = head_dim // 2
    frequency = jnp.exp(-jnp.log(THETA) * 2.0 * jnp.arange(half_dim, dtype=F32) / head_dim)
    angles = jnp.arange(length, dtype=F32)[:, None] * frequency[None, :]
    cosine, sine = jnp.cos(angles), jnp.sin(angles)
    return jnp.concatenate([cosine, cosine], axis=1), jnp.concatenate([-sine, sine], axis=1)


def dot(a, b):
    return jnp.dot(a, b, preferred_element_type=F32)


def dot_nt(a, b):
    return lax.dot_general(a, b, (((1,), (1,)), ((), ())), preferred_element_type=F32)


def dot_tn(a, b):
    return lax.dot_general(a, b, (((0,), (0,)), ((), ())), preferred_element_type=F32)


class Plan:
    def __init__(self, length, slots, n_columns, n_owners):
        self.length, self.slots = length, slots
        self.n_owners = n_owners
        self.q_heads = HQ // n_columns
        self.kv_heads = HK // n_columns
        self.group = self.q_heads // self.kv_heads
        self.q_end = self.q_heads * HD
        self.k_end = self.q_end + self.kv_heads * HD
        self.width = self.k_end + self.kv_heads * HD
        self.qkv_cols = self.width // BLK
        self.d_blocks = D // BLK
        self.split = self.d_blocks * self.qkv_cols
        self.total = self.split + self.q_end // BLK * self.d_blocks
        self.rows = min(256, length)
        evens = list(range(0, n_owners, 2))
        odds = list(range(1, n_owners, 2))[::-1]
        self.order = evens + odds
        cuts = [slots * k // STREAMS for k in range(STREAMS + 1)]
        self.streams = [
            (1 if k < STREAMS // 2 else -1, cuts[k], cuts[k + 1]) for k in range(STREAMS)
        ]
        n = n_owners
        self.forward = [(self.order[i], self.order[(i + 1) % n]) for i in range(n)]
        self.backward = [(b, a) for a, b in self.forward]

    def perm(self, direction):
        return self.forward if direction > 0 else self.backward


def gather_ring(plan, chunk):
    pieces = [[chunk[lo:hi]] for _, lo, hi in plan.streams]
    for step in range(1, plan.n_owners):
        for k, (direction, _, _) in enumerate(plan.streams):
            pieces[k].append(lax.ppermute(pieces[k][step - 1], "fsdp", plan.perm(direction)))
    return pieces


def reduce_ring(plan, pieces, factor):
    n = plan.n_owners
    held = [pieces[k][1] for k in range(len(plan.streams))]
    for step in range(2, n + 1):
        for k, (direction, _, _) in enumerate(plan.streams):
            arrived = lax.ppermute(held[k], "fsdp", plan.perm(direction))
            own = pieces[k][step % n]
            if step < n:
                held[k] = arrived + own
            else:
                held[k] = (arrived.astype(F32) + own.astype(F32)) * factor
    return jnp.concatenate(held, axis=0)


def loop_blocks(plan, table, k, step, lo, hi, on_qkv, on_out):
    row = 0 if plan.streams[k][0] > 0 else 2
    start, count = table[row, step], table[row + 1, step]

    def visit(t, carry):
        block = start + t

        @pl.when(block < plan.split)
        def _():
            on_qkv(t - lo, lax.div(block, plan.qkv_cols), lax.rem(block, plan.qkv_cols))

        @pl.when(block >= plan.split)
        def _():
            rest = block - plan.split
            on_out(t - lo, lax.div(rest, plan.d_blocks), lax.rem(rest, plan.d_blocks))

        return carry

    lax.fori_loop(lo, jnp.minimum(hi, count), visit, 0)


def tile(ref, row, col):
    return ref.at[
        pl.ds(pl.multiple_of(row * BLK, BLK), BLK), pl.ds(pl.multiple_of(col * BLK, BLK), BLK)
    ]


def unpack(plan, table, refs, qkv, out, qkv_sem, out_sem):
    at = 0
    for k, (_, lo, hi) in enumerate(plan.streams):
        for step in range(plan.n_owners):
            ref = refs[at]
            at += 1
            loop_blocks(
                plan, table, k, step, lo, hi,
                lambda t, r, c, ref=ref: pltpu.make_async_copy(ref.at[t], tile(qkv, r, c), qkv_sem).start(),
                lambda t, r, c, ref=ref: pltpu.make_async_copy(ref.at[t], tile(out, r, c), out_sem).start(),
            )


def wait_all(ref, sem):
    pltpu.make_async_copy(ref, ref, sem).wait()


def turn(x, cosine, sine):
    return x * cosine + pltpu.roll(x, HD // 2, 1) * sine


def softmax_rows(plan, q, keys, first, end):
    scores = dot_nt(q, keys) * HD ** (-0.5)
    rows = lax.broadcasted_iota(jnp.int32, scores.shape, 0) + first
    cols = lax.broadcasted_iota(jnp.int32, scores.shape, 1)
    scores = jnp.where(rows >= cols, scores, NEGATIVE)
    scores = jnp.exp(scores - jnp.max(scores, axis=1, keepdims=True))
    return scores / jnp.sum(scores, axis=1, keepdims=True)


def heads(plan):
    for head in range(plan.q_heads):
        kv = head // plan.group
        yield (
            slice(head * HD, (head + 1) * HD),
            slice(plan.q_end + kv * HD, plan.q_end + (kv + 1) * HD),
            slice(plan.k_end + kv * HD, plan.k_end + (kv + 1) * HD),
        )


def row_blocks(plan):
    return [(first, first + plan.rows) for first in range(0, plan.length, plan.rows)]


def project(plan, normed, matrix, result):
    cosine, sine, sink = result[1], result[2], result[0]
    step = 2 * HD
    for first in range(0, plan.width, step):
        end = min(first + step, plan.width)
        part = dot(normed[...], matrix[:, first:end])
        for at in range(first, end, HD):
            piece = part[:, at - first : at - first + HD]
            if at < plan.k_end:
                piece = turn(piece, cosine[...], sine[...])
            sink[:, at : at + HD] = piece.astype(BF16)


def weight_kernel(plan, table, normed, cosine, sine, *rest):
    n_refs = len(plan.streams) * plan.n_owners
    refs = rest[:n_refs]
    fields, mixed, w_out, w_qkv, qkv_sem, out_sem = rest[n_refs:]
    unpack(plan, table, refs, w_qkv, w_out, qkv_sem, out_sem)
    wait_all(w_qkv, qkv_sem)
    project(plan, normed, w_qkv, (fields, cosine, sine))
    for q_at, k_at, v_at in heads(plan):
        for first, end in row_blocks(plan):
            probs = softmax_rows(plan, fields[first:end, q_at], fields[:end, k_at], first, end)
            mixed[first:end, q_at] = dot(probs.astype(BF16), fields[:end, v_at]).astype(BF16)
    wait_all(w_out, out_sem)


def probe_kernel(plan, table, normed, cosine, sine, fields, mixed, w_out, *rest):
    n_refs = len(plan.streams) * plan.n_owners
    refs = rest[:n_refs]
    tangent, p_qkv, p_out, moved, mixed_moved, qkv_sem, out_sem = rest[n_refs:]
    unpack(plan, table, refs, p_qkv, p_out, qkv_sem, out_sem)
    wait_all(p_qkv, qkv_sem)
    project(plan, normed, p_qkv, (moved, cosine, sine))
    for q_at, k_at, v_at in heads(plan):
        for first, end in row_blocks(plan):
            q, dq = fields[first:end, q_at], moved[first:end, q_at]
            keys, d_keys = fields[:end, k_at], moved[:end, k_at]
            values, d_values = fields[:end, v_at], moved[:end, v_at]
            probs = softmax_rows(plan, q, keys, first, end)
            d_scores = (dot_nt(dq, keys) + dot_nt(q, d_keys)) * HD ** (-0.5)
            d_probs = probs * (d_scores - jnp.sum(probs * d_scores, axis=1, keepdims=True))
            mixed_moved[first:end, q_at] = (
                dot(d_probs.astype(BF16), values) + dot(probs.astype(BF16), d_values)
            ).astype(BF16)
    wait_all(p_out, out_sem)
    step = 2 * BLK

    def columns(i, carry):
        at = pl.ds(pl.multiple_of(i * step, step), step)
        tangent[:, at] = (
            dot(mixed_moved[...], w_out[:, at]) + dot(mixed[...], p_out[:, at])
        ).astype(BF16)
        return carry

    lax.fori_loop(0, D // step, columns, 0)


def pull_kernel(plan, table, weighted, normed_t, w_out_t, fields, mixed_t, cosine, sine, *rest):
    n_refs = len(plan.streams) * plan.n_owners
    refs = rest[:n_refs]
    g_qkv, g_out, d_mixed, d_proj, qkv_sem, out_sem = rest[n_refs:]
    step = 2 * BLK

    def columns(i, carry):
        at = pl.ds(pl.multiple_of(i * step, step), step)
        g_out[:, at] = dot(mixed_t[...], weighted[:, at]).astype(BF16)
        return carry

    lax.fori_loop(0, D // step, columns, 0)
    d_mixed[...] = dot(weighted[...], w_out_t[...]).astype(BF16)
    ends = row_blocks(plan)
    scale = HD ** (-0.5)
    for kv in range(plan.kv_heads):
        d_keys = [None] * len(ends)
        d_values = [None] * len(ends)
        for head, (q_at, k_at, v_at) in enumerate(heads(plan)):
            if head // plan.group != kv:
                continue
            for i, (first, end) in enumerate(ends):
                q, d_mix = fields[first:end, q_at], d_mixed[first:end, q_at]
                keys, values = fields[:end, k_at], fields[:end, v_at]
                probs = softmax_rows(plan, q, keys, first, end)
                d_probs = dot_nt(d_mix, values).astype(BF16).astype(F32)
                d_scores = probs * (d_probs - jnp.sum(probs * d_probs, axis=1, keepdims=True))
                d_scores = (d_scores * scale).astype(BF16)
                d_q = dot(d_scores, keys).astype(BF16).astype(F32)
                d_proj[first:end, q_at] = turn(
                    d_q, cosine[first:end, :], -sine[first:end, :]
                ).astype(BF16)
                add_k, add_v = dot_tn(d_scores, q), dot_tn(probs.astype(BF16), d_mix)
                for j in range(i + 1):
                    lo, hi = ends[j]
                    d_keys[j] = add_k[lo:hi] if d_keys[j] is None else d_keys[j] + add_k[lo:hi]
                    d_values[j] = add_v[lo:hi] if d_values[j] is None else d_values[j] + add_v[lo:hi]
        for j, (lo, hi) in enumerate(ends):
            d_proj[lo:hi, k_at] = turn(
                d_keys[j].astype(BF16).astype(F32), cosine[lo:hi, :], -sine[lo:hi, :]
            ).astype(BF16)
            d_proj[lo:hi, v_at] = d_values[j].astype(BF16)
    rows = 4 * BLK

    def qkv_rows(i, carry):
        at = pl.ds(pl.multiple_of(i * rows, rows), rows)
        g_qkv[at, :] = dot(normed_t[at, :], d_proj[...]).astype(BF16)
        return carry

    lax.fori_loop(0, D // rows, qkv_rows, 0)
    at = 0
    for k, (_, lo, hi) in enumerate(plan.streams):
        for step in range(plan.n_owners):
            ref = refs[at]
            at += 1
            loop_blocks(
                plan, table, k, step, lo, hi,
                lambda t, r, c, ref=ref: pltpu.make_async_copy(tile(g_qkv, r, c), ref.at[t], qkv_sem).start(),
                lambda t, r, c, ref=ref: pltpu.make_async_copy(tile(g_out, r, c), ref.at[t], out_sem).start(),
            )
    wait_all(g_qkv, qkv_sem)
    wait_all(g_out, out_sem)


VMEM = pl.BlockSpec(memory_space=pltpu.VMEM)
SMEM = pl.BlockSpec(memory_space=pltpu.SMEM)
ANY = pl.BlockSpec(memory_space=pl.ANY)
PARAMS = pltpu.CompilerParams(vmem_limit_bytes=58 * 1024 * 1024)


def flat(pieces):
    return [piece for stream in pieces for piece in stream]


def local(tokens, norm_gain, curvature, weight_slots, probe_slots, block_counts):
    n_columns = lax.axis_size("seq")
    n_owners = lax.axis_size("fsdp")
    slots = weight_slots.shape[1]
    length = tokens.shape[1]
    plan = Plan(length, slots, n_columns, n_owners)
    counts = block_counts[0]
    range_ends = jnp.cumsum(counts)
    starts = range_ends - counts
    me = lax.axis_index("fsdp")
    order = jnp.array(plan.order, jnp.int32)
    owner_ids = jnp.arange(n_owners, dtype=jnp.int32)
    place = jnp.sum(jnp.where(order == me, owner_ids, 0))
    behind = order[(place - owner_ids) % n_owners]
    ahead = order[(place + owner_ids) % n_owners]
    table = jnp.stack([starts[behind], counts[behind], starts[ahead], counts[ahead]]).astype(jnp.int32)

    w_pieces = gather_ring(plan, weight_slots[0])
    p_pieces = gather_ring(plan, probe_slots[0])

    values = tokens[0].astype(F32)
    factor = lax.rsqrt(jnp.mean(values * values, axis=-1, keepdims=True) + EPS)
    normed = (values * factor * norm_gain).astype(BF16)
    cosine, sine = rotary(length, HD)
    sem = pltpu.SemaphoreType.DMA
    n_refs = len(plan.streams) * n_owners

    def kernel(body):
        return lambda *refs: body(plan, *refs)

    fields, mixed, w_out = pl.pallas_call(
        kernel(weight_kernel),
        out_shape=[
            jax.ShapeDtypeStruct((length, plan.width), BF16),
            jax.ShapeDtypeStruct((length, plan.q_end), BF16),
            jax.ShapeDtypeStruct((plan.q_end, D), BF16),
        ],
        in_specs=[SMEM] + [VMEM] * 3 + [ANY] * n_refs,
        out_specs=[VMEM] * 3,
        scratch_shapes=[pltpu.VMEM((D, plan.width), BF16), sem, sem],
        compiler_params=PARAMS,
        name="weights",
    )(table, normed, cosine, sine, *flat(w_pieces))
    tangent = pl.pallas_call(
        kernel(probe_kernel),
        out_shape=jax.ShapeDtypeStruct((length, D), BF16),
        in_specs=[SMEM] + [VMEM] * 6 + [ANY] * n_refs,
        out_specs=VMEM,
        scratch_shapes=[
            pltpu.VMEM((D, plan.width), BF16),
            pltpu.VMEM((plan.q_end, D), BF16),
            pltpu.VMEM((length, plan.width), BF16),
            pltpu.VMEM((length, plan.q_end), BF16),
            sem,
            sem,
        ],
        compiler_params=PARAMS,
        name="probe",
    )(table, normed, cosine, sine, fields, mixed, w_out, *flat(p_pieces))
    share = lax.psum_scatter(tangent, "seq", scatter_dimension=1, tiled=True).astype(F32)
    share_width = share.shape[1]
    curv_share = lax.dynamic_slice_in_dim(
        curvature[0], lax.axis_index("seq") * share_width, share_width, 1
    )
    weighted_share = (curv_share.astype(F32) * share).astype(BF16)
    weighted = lax.all_gather(weighted_share, "seq", axis=1, tiled=True)

    pieces = pl.pallas_call(
        kernel(pull_kernel),
        out_shape=[
            jax.ShapeDtypeStruct((hi - lo, BLK, BLK), BF16)
            for _, lo, hi in plan.streams
            for _ in range(n_owners)
        ],
        in_specs=[SMEM] + [VMEM] * 7,
        out_specs=[ANY] * n_refs,
        scratch_shapes=[
            pltpu.VMEM((D, plan.width), BF16),
            pltpu.VMEM((plan.q_end, D), BF16),
            pltpu.VMEM((length, plan.q_end), BF16),
            pltpu.VMEM((length, plan.width), BF16),
            sem,
            sem,
        ],
        compiler_params=PARAMS,
        name="pull",
    )(table, weighted, normed.T, w_out.T, fields, mixed.T, cosine, sine)
    pieces = [pieces[k * n_owners : (k + 1) * n_owners] for k in range(len(plan.streams))]
    summed = reduce_ring(plan, pieces, 1.0 / jnp.sqrt(F32(length * n_owners)))
    live = jnp.arange(slots, dtype=jnp.int32) < counts[me]
    return jnp.where(live[:, None, None], summed, 0.0)[None]


def solution(mesh):
    in_specs = (
        P("fsdp", None, None),
        P(),
        P("fsdp", None, None),
        P("seq", "fsdp", None, None),
        P("seq", "fsdp", None, None),
        P("seq", None),
    )
    out_specs = P("seq", "fsdp", None, None)
    return jax.shard_map(local, mesh=mesh, in_specs=in_specs, out_specs=out_specs, check_vma=False)
```

```python
import jax
import jax.numpy as jnp
from jax import lax
from jax.experimental import pallas as pl
from jax.experimental.pallas import tpu as pltpu
from jax.sharding import PartitionSpec as P

D = 4096
HQ = 16
HK = 4
HD = 128
BLK = 128

THETA = 500000.0
EPS = 1e-05
NEGATIVE = -1e30

STREAMS = 4
F32 = jnp.float32
BF16 = jnp.bfloat16


def rotary(length, head_dim):
    half_dim = head_dim // 2
    frequency = jnp.exp(-jnp.log(THETA) * 2.0 * jnp.arange(half_dim, dtype=F32) / head_dim)
    angles = jnp.arange(length, dtype=F32)[:, None] * frequency[None, :]
    cosine, sine = jnp.cos(angles), jnp.sin(angles)
    return jnp.concatenate([cosine, cosine], axis=1), jnp.concatenate([-sine, sine], axis=1)


def dot(a, b):
    return jnp.dot(a, b, preferred_element_type=F32)


def dot_nt(a, b):
    return lax.dot_general(a, b, (((1,), (1,)), ((), ())), preferred_element_type=F32)


def dot_tn(a, b):
    return lax.dot_general(a, b, (((0,), (0,)), ((), ())), preferred_element_type=F32)


class Plan:
    def __init__(self, length, slots, n_columns, n_owners):
        self.length, self.slots = length, slots
        self.n_owners = n_owners
        self.q_heads = HQ // n_columns
        self.kv_heads = HK // n_columns
        self.group = self.q_heads // self.kv_heads
        self.q_end = self.q_heads * HD
        self.k_end = self.q_end + self.kv_heads * HD
        self.width = self.k_end + self.kv_heads * HD
        self.qkv_cols = self.width // BLK
        self.d_blocks = D // BLK
        self.split = self.d_blocks * self.qkv_cols
        self.total = self.split + self.q_end // BLK * self.d_blocks
        self.rows = min(256, length)
        evens = list(range(0, n_owners, 2))
        odds = list(range(1, n_owners, 2))[::-1]
        self.order = evens + odds
        cuts = [slots * k // STREAMS for k in range(STREAMS + 1)]
        self.streams = [
            (1 if k < STREAMS // 2 else -1, cuts[k], cuts[k + 1]) for k in range(STREAMS)
        ]
        n = n_owners
        self.forward = [(self.order[i], self.order[(i + 1) % n]) for i in range(n)]
        self.backward = [(b, a) for a, b in self.forward]

    def perm(self, direction):
        return self.forward if direction > 0 else self.backward


def tie_kernel(*refs):
    pass


def tie(x, *after):
    return pl.pallas_call(
        tie_kernel,
        out_shape=jax.ShapeDtypeStruct(x.shape, x.dtype),
        in_specs=[ANY] * (1 + len(after)),
        out_specs=ANY,
        input_output_aliases={0: 0},
        name="tie",
    )(x, *after)


def gather_ring(plan, chunk, after=None, during=None):
    pieces = [[chunk[lo:hi]] for _, lo, hi in plan.streams]
    heads_of = [stream[0] for stream in pieces]
    if after is not None:
        heads_of = [tie(x, after[k]) for k, x in enumerate(heads_of)]
    for step in range(1, plan.n_owners):
        for k, (direction, _, _) in enumerate(plan.streams):
            last = heads_of[k] if step == 1 else pieces[k][step - 1]
            if during and k == 0 and step in during:
                last = tie(last, *during[step])
            pieces[k].append(lax.ppermute(last, "fsdp", plan.perm(direction)))
    return pieces


def reduce_ring(plan, pieces, factor):
    n = plan.n_owners
    held = [pieces[k][1] for k in range(len(plan.streams))]
    for step in range(2, n + 1):
        for k, (direction, _, _) in enumerate(plan.streams):
            arrived = lax.ppermute(held[k], "fsdp", plan.perm(direction))
            own = pieces[k][step % n]
            if step < n:
                held[k] = arrived + own
            else:
                held[k] = (arrived.astype(F32) + own.astype(F32)) * factor
    return jnp.concatenate(held, axis=0)


def swap(x, bit, n):
    return lax.ppermute(x, "seq", [(i, i ^ bit) for i in range(n)])


def reduce_columns(parts, n):
    parts = dict(enumerate(parts))
    bit = 1
    while 2 * bit < n:
        for r in [r for r in parts if r & bit]:
            parts[r ^ bit] = parts[r ^ bit] + swap(parts.pop(r), bit, n)
        bit *= 2
    return parts[0], swap(parts[bit], bit, n)


def gather_columns(share, n):
    parts = {0: share}
    bit = n // 2
    while bit:
        for r in list(parts):
            parts[r ^ bit] = swap(parts[r], bit, n)
        bit //= 2
    return [parts[r] for r in range(n)]


def loop_blocks(plan, table, k, step, lo, hi, on_qkv, on_out):
    row = 0 if plan.streams[k][0] > 0 else 2
    start, count = table[row, step], table[row + 1, step]

    def visit(t, carry):
        block = start + t

        @pl.when(block < plan.split)
        def _():
            on_qkv(t - lo, lax.div(block, plan.qkv_cols), lax.rem(block, plan.qkv_cols))

        @pl.when(block >= plan.split)
        def _():
            rest = block - plan.split
            on_out(t - lo, lax.div(rest, plan.d_blocks), lax.rem(rest, plan.d_blocks))

        return carry

    lax.fori_loop(lo, jnp.minimum(hi, count), visit, 0)


def tile(ref, row, col):
    return ref.at[
        pl.ds(pl.multiple_of(row * BLK, BLK), BLK), pl.ds(pl.multiple_of(col * BLK, BLK), BLK)
    ]


def unpack(plan, table, refs, qkv, out, qkv_sem, out_sem):
    at = 0
    for k, (_, lo, hi) in enumerate(plan.streams):
        for step in range(plan.n_owners):
            ref = refs[at]
            at += 1
            loop_blocks(
                plan, table, k, step, lo, hi,
                lambda t, r, c, ref=ref: pltpu.make_async_copy(ref.at[t], tile(qkv, r, c), qkv_sem).start(),
                lambda t, r, c, ref=ref: pltpu.make_async_copy(ref.at[t], tile(out, r, c), out_sem).start(),
            )


def wait_all(ref, sem):
    pltpu.make_async_copy(ref, ref, sem).wait()


def turn(x, cosine, sine):
    return x * cosine + pltpu.roll(x, HD // 2, 1) * sine


def softmax_rows(plan, q, keys, first, end):
    scores = dot_nt(q, keys) * HD ** (-0.5)
    rows = lax.broadcasted_iota(jnp.int32, scores.shape, 0) + first
    cols = lax.broadcasted_iota(jnp.int32, scores.shape, 1)
    scores = jnp.where(rows >= cols, scores, NEGATIVE)
    scores = jnp.exp(scores - jnp.max(scores, axis=1, keepdims=True))
    return scores / jnp.sum(scores, axis=1, keepdims=True)


def heads(plan):
    for head in range(plan.q_heads):
        kv = head // plan.group
        yield (
            slice(head * HD, (head + 1) * HD),
            slice(plan.q_end + kv * HD, plan.q_end + (kv + 1) * HD),
            slice(plan.k_end + kv * HD, plan.k_end + (kv + 1) * HD),
        )


def row_blocks(plan):
    return [(first, first + plan.rows) for first in range(0, plan.length, plan.rows)]


def project(plan, normed, matrix, result):
    cosine, sine, sink = result[1], result[2], result[0]
    step = 2 * HD
    for first in range(0, plan.width, step):
        end = min(first + step, plan.width)
        part = dot(normed[...], matrix[:, first:end])
        for at in range(first, end, HD):
            piece = part[:, at - first : at - first + HD]
            if at < plan.k_end:
                piece = turn(piece, cosine[...], sine[...])
            sink[:, at : at + HD] = piece.astype(BF16)


def weight_kernel(plan, table, normed, cosine, sine, *rest):
    n_refs = len(plan.streams) * plan.n_owners
    refs = rest[:n_refs]
    fields, w_out, w_qkv, qkv_sem, out_sem = rest[n_refs:]
    unpack(plan, table, refs, w_qkv, w_out, qkv_sem, out_sem)
    wait_all(w_qkv, qkv_sem)
    project(plan, normed, w_qkv, (fields, cosine, sine))
    wait_all(w_out, out_sem)


def mix_kernel(plan, fields, mixed):
    for q_at, k_at, v_at in heads(plan):
        for first, end in row_blocks(plan):
            probs = softmax_rows(plan, fields[first:end, q_at], fields[:end, k_at], first, end)
            mixed[first:end, q_at] = dot(probs.astype(BF16), fields[:end, v_at]).astype(BF16)


def probe_kernel(plan, shares, table, normed, cosine, sine, fields, mixed, w_out, *rest):
    n_refs = len(plan.streams) * plan.n_owners
    refs = rest[:n_refs]
    tangents = rest[n_refs : n_refs + shares * len(row_blocks(plan))]
    p_qkv, p_out, moved, mixed_moved, qkv_sem, out_sem = rest[n_refs + len(tangents) :]
    unpack(plan, table, refs, p_qkv, p_out, qkv_sem, out_sem)
    wait_all(p_qkv, qkv_sem)
    project(plan, normed, p_qkv, (moved, cosine, sine))
    for q_at, k_at, v_at in heads(plan):
        for first, end in row_blocks(plan):
            q, dq = fields[first:end, q_at], moved[first:end, q_at]
            keys, d_keys = fields[:end, k_at], moved[:end, k_at]
            values, d_values = fields[:end, v_at], moved[:end, v_at]
            probs = softmax_rows(plan, q, keys, first, end)
            d_scores = (dot_nt(dq, keys) + dot_nt(q, d_keys)) * HD ** (-0.5)
            d_probs = probs * (d_scores - jnp.sum(probs * d_scores, axis=1, keepdims=True))
            mixed_moved[first:end, q_at] = (
                dot(d_probs.astype(BF16), values) + dot(probs.astype(BF16), d_values)
            ).astype(BF16)
    wait_all(p_out, out_sem)
    step = 2 * BLK
    share = D // shares
    ends = row_blocks(plan)
    for r in range(shares):
        base = (table[4, 0] ^ r) * share

        def columns(i, carry, r=r, base=base):
            here = pl.ds(pl.multiple_of(i * step, step), step)
            there = pl.ds(pl.multiple_of(base + i * step, step), step)
            part = dot(mixed_moved[...], w_out[:, there]) + dot(mixed[...], p_out[:, there])
            for j, (first, end) in enumerate(ends):
                tangents[j * shares + r][:, here] = part[first:end].astype(BF16)
            return carry

        lax.fori_loop(0, share // step, columns, 0)


def pull_kernel(plan, shares, table, normed_t, w_out_t, fields, mixed_t, cosine, sine, *rest):
    ends = row_blocks(plan)
    weighted = rest[: shares * len(ends)]
    n_refs = len(plan.streams) * plan.n_owners
    refs = rest[len(weighted) : len(weighted) + n_refs]
    g_qkv, g_out, d_mixed, d_proj, qkv_sem, out_sem = rest[len(weighted) + n_refs :]
    step = 2 * BLK
    share = D // shares
    total = [None] * len(ends)
    for r in range(shares):
        base = (table[4, 0] ^ r) * share
        for j, (first, end) in enumerate(ends):
            part = dot(weighted[j * shares + r][...], w_out_t[pl.ds(pl.multiple_of(base, share), share), :])
            total[j] = part if total[j] is None else total[j] + part
    for j, (first, end) in enumerate(ends):
        d_mixed[first:end, :] = total[j].astype(BF16)
    for r in range(shares):
        base = (table[4, 0] ^ r) * share

        def columns(i, carry, r=r, base=base):
            here = pl.ds(pl.multiple_of(i * step, step), step)
            there = pl.ds(pl.multiple_of(base + i * step, step), step)
            part = None
            for j, (first, end) in enumerate(ends):
                more = dot(mixed_t[:, first:end], weighted[j * shares + r][:, here])
                part = more if part is None else part + more
            g_out[:, there] = part.astype(BF16)
            return carry

        lax.fori_loop(0, share // step, columns, 0)
    scale = HD ** (-0.5)
    for kv in range(plan.kv_heads):
        d_keys = [None] * len(ends)
        d_values = [None] * len(ends)
        for head, (q_at, k_at, v_at) in enumerate(heads(plan)):
            if head // plan.group != kv:
                continue
            k_here, v_here = k_at, v_at
            for i, (first, end) in enumerate(ends):
                q, d_mix = fields[first:end, q_at], d_mixed[first:end, q_at]
                keys, values = fields[:end, k_at], fields[:end, v_at]
                probs = softmax_rows(plan, q, keys, first, end)
                d_probs = dot_nt(d_mix, values).astype(BF16).astype(F32)
                d_scores = probs * (d_probs - jnp.sum(probs * d_probs, axis=1, keepdims=True))
                d_scores = (d_scores * scale).astype(BF16)
                d_q = dot(d_scores, keys).astype(BF16).astype(F32)
                d_proj[first:end, q_at] = turn(
                    d_q, cosine[first:end, :], -sine[first:end, :]
                ).astype(BF16)
                add_k, add_v = dot_tn(d_scores, q), dot_tn(probs.astype(BF16), d_mix)
                for j in range(i + 1):
                    lo, hi = ends[j]
                    d_keys[j] = add_k[lo:hi] if d_keys[j] is None else d_keys[j] + add_k[lo:hi]
                    d_values[j] = add_v[lo:hi] if d_values[j] is None else d_values[j] + add_v[lo:hi]
        for j, (lo, hi) in enumerate(ends):
            d_proj[lo:hi, k_here] = turn(
                d_keys[j].astype(BF16).astype(F32), cosine[lo:hi, :], -sine[lo:hi, :]
            ).astype(BF16)
            d_proj[lo:hi, v_here] = d_values[j].astype(BF16)
    rows = 4 * BLK

    def qkv_rows(i, carry):
        at = pl.ds(pl.multiple_of(i * rows, rows), rows)
        g_qkv[at, :] = dot(normed_t[at, :], d_proj[...]).astype(BF16)
        return carry

    lax.fori_loop(0, D // rows, qkv_rows, 0)
    at = 0
    for k, (_, lo, hi) in enumerate(plan.streams):
        for step in range(plan.n_owners):
            ref = refs[at]
            at += 1
            loop_blocks(
                plan, table, k, step, lo, hi,
                lambda t, r, c, ref=ref: pltpu.make_async_copy(tile(g_qkv, r, c), ref.at[t], qkv_sem).start(),
                lambda t, r, c, ref=ref: pltpu.make_async_copy(tile(g_out, r, c), ref.at[t], out_sem).start(),
            )
    wait_all(g_qkv, qkv_sem)
    wait_all(g_out, out_sem)


VMEM = pl.BlockSpec(memory_space=pltpu.VMEM)
SMEM = pl.BlockSpec(memory_space=pltpu.SMEM)
ANY = pl.BlockSpec(memory_space=pl.ANY)
PARAMS = pltpu.CompilerParams(vmem_limit_bytes=58 * 1024 * 1024)


def flat(pieces):
    return [piece for stream in pieces for piece in stream]


def local(tokens, norm_gain, curvature, weight_slots, probe_slots, block_counts):
    n_columns = lax.axis_size("seq")
    n_owners = lax.axis_size("fsdp")
    slots = weight_slots.shape[1]
    length = tokens.shape[1]
    plan = Plan(length, slots, n_columns, n_owners)
    counts = block_counts[0]
    range_ends = jnp.cumsum(counts)
    starts = range_ends - counts
    me = lax.axis_index("fsdp")
    column = lax.axis_index("seq")
    order = jnp.array(plan.order, jnp.int32)
    owner_ids = jnp.arange(n_owners, dtype=jnp.int32)
    place = jnp.sum(jnp.where(order == me, owner_ids, 0))
    behind = order[(place - owner_ids) % n_owners]
    ahead = order[(place + owner_ids) % n_owners]
    own_column = jnp.full((n_owners,), column, jnp.int32)
    table = jnp.stack(
        [starts[behind], counts[behind], starts[ahead], counts[ahead], own_column]
    ).astype(jnp.int32)

    n = n_owners
    w_pieces = gather_ring(plan, weight_slots[0])
    values = tokens[0].astype(F32)
    factor = lax.rsqrt(jnp.mean(values * values, axis=-1, keepdims=True) + EPS)
    normed = (values * factor * norm_gain).astype(BF16)
    cosine, sine = rotary(length, HD)
    sem = pltpu.SemaphoreType.DMA
    halves = len(row_blocks(plan))
    share = D // n_columns

    n_refs = len(plan.streams) * n
    fields, w_out = pl.pallas_call(
        lambda *refs: weight_kernel(plan, *refs),
        out_shape=[
            jax.ShapeDtypeStruct((length, plan.width), BF16),
            jax.ShapeDtypeStruct((plan.q_end, D), BF16),
        ],
        in_specs=[SMEM] + [VMEM] * 3 + [ANY] * n_refs,
        out_specs=[VMEM] * 2,
        scratch_shapes=[pltpu.VMEM((D, plan.width), BF16), sem, sem],
        compiler_params=PARAMS,
        name="weights",
    )(table, normed, cosine, sine, *flat(w_pieces))
    mixed = pl.pallas_call(
        lambda *refs: mix_kernel(plan, *refs),
        out_shape=jax.ShapeDtypeStruct((length, plan.q_end), BF16),
        in_specs=[VMEM],
        out_specs=VMEM,
        compiler_params=PARAMS,
        name="mix",
    )(fields)
    p_pieces = gather_ring(
        plan, probe_slots[0], [stream[n - 2] for stream in w_pieces], {2: (fields,), 4: (mixed,)}
    )
    tangents = pl.pallas_call(
        lambda *refs: probe_kernel(plan, n_columns, *refs),
        out_shape=[jax.ShapeDtypeStruct((plan.rows, share), BF16)] * (halves * n_columns),
        in_specs=[SMEM] + [VMEM] * 6 + [ANY] * n_refs,
        out_specs=[VMEM] * (halves * n_columns),
        scratch_shapes=[
            pltpu.VMEM((D, plan.width), BF16),
            pltpu.VMEM((plan.q_end, D), BF16),
            pltpu.VMEM((length, plan.width), BF16),
            pltpu.VMEM((length, plan.q_end), BF16),
            sem,
            sem,
        ],
        compiler_params=PARAMS,
        name="probe",
    )(table, normed, cosine, sine, fields, mixed, w_out, *flat(p_pieces))
    curv_share = lax.dynamic_slice_in_dim(curvature[0], column * share, share, 1)
    weighted = []
    for j, (first, end) in enumerate(row_blocks(plan)):
        own, other = reduce_columns(tangents[j * n_columns : (j + 1) * n_columns], n_columns)
        total = own.astype(F32) + other.astype(F32)
        mine = (curv_share[first:end].astype(F32) * total).astype(BF16)
        weighted += gather_columns(mine, n_columns)

    pieces = pl.pallas_call(
        lambda *refs: pull_kernel(plan, n_columns, *refs),
        out_shape=[
            jax.ShapeDtypeStruct((hi - lo, BLK, BLK), BF16)
            for _, lo, hi in plan.streams
            for _ in range(n)
        ],
        in_specs=[SMEM] + [VMEM] * (6 + halves * n_columns),
        out_specs=[ANY] * n_refs,
        scratch_shapes=[
            pltpu.VMEM((D, plan.width), BF16),
            pltpu.VMEM((plan.q_end, D), BF16),
            pltpu.VMEM((length, plan.q_end), BF16),
            pltpu.VMEM((length, plan.width), BF16),
            sem,
            sem,
        ],
        compiler_params=PARAMS,
        name="pull",
    )(table, normed.T, w_out.T, fields, mixed.T, cosine, sine, *weighted)

    pieces = [pieces[k * n : (k + 1) * n] for k in range(len(plan.streams))]
    summed = reduce_ring(plan, pieces, 1.0 / jnp.sqrt(F32(length * n_owners)))
    live = jnp.arange(slots, dtype=jnp.int32) < counts[me]
    return jnp.where(live[:, None, None], summed, 0.0)[None]


def solution(mesh):
    in_specs = (
        P("fsdp", None, None),
        P(),
        P("fsdp", None, None),
        P("seq", "fsdp", None, None),
        P("seq", "fsdp", None, None),
        P("seq", None),
    )
    out_specs = P("seq", "fsdp", None, None)
    return jax.shard_map(local, mesh=mesh, in_specs=in_specs, out_specs=out_specs, check_vma=False)
```

```python
import jax
import jax.numpy as jnp
from jax import lax
from jax.experimental import pallas as pl
from jax.experimental.pallas import tpu as pltpu
from jax.sharding import PartitionSpec as P

D = 4096
HQ = 16
HK = 4
HD = 128
BLK = 128

THETA = 500000.0
EPS = 1e-05
NEGATIVE = -1e30

STREAMS = 4
F32 = jnp.float32
BF16 = jnp.bfloat16


def rotary(length, head_dim):
    half_dim = head_dim // 2
    frequency = jnp.exp(-jnp.log(THETA) * 2.0 * jnp.arange(half_dim, dtype=F32) / head_dim)
    angles = jnp.arange(length, dtype=F32)[:, None] * frequency[None, :]
    cosine, sine = jnp.cos(angles), jnp.sin(angles)
    return jnp.concatenate([cosine, cosine], axis=1), jnp.concatenate([-sine, sine], axis=1)


def dot(a, b):
    return jnp.dot(a, b, preferred_element_type=F32)


def dot_nt(a, b):
    return lax.dot_general(a, b, (((1,), (1,)), ((), ())), preferred_element_type=F32)


def dot_tn(a, b):
    return lax.dot_general(a, b, (((0,), (0,)), ((), ())), preferred_element_type=F32)


class Plan:
    def __init__(self, length, slots, n_columns, n_owners):
        self.length, self.slots = length, slots
        self.n_owners = n_owners
        self.q_heads = HQ // n_columns
        self.kv_heads = HK // n_columns
        self.group = self.q_heads // self.kv_heads
        self.q_end = self.q_heads * HD
        self.k_end = self.q_end + self.kv_heads * HD
        self.width = self.k_end + self.kv_heads * HD
        self.qkv_cols = self.width // BLK
        self.d_blocks = D // BLK
        self.split = self.d_blocks * self.qkv_cols
        self.total = self.split + self.q_end // BLK * self.d_blocks
        self.rows = min(256, length)
        evens = list(range(0, n_owners, 2))
        odds = list(range(1, n_owners, 2))[::-1]
        self.order = evens + odds
        cuts = [slots * k // STREAMS for k in range(STREAMS + 1)]
        self.streams = [
            (1 if k < STREAMS // 2 else -1, cuts[k], cuts[k + 1]) for k in range(STREAMS)
        ]
        n = n_owners
        self.forward = [(self.order[i], self.order[(i + 1) % n]) for i in range(n)]
        self.backward = [(b, a) for a, b in self.forward]

    def perm(self, direction):
        return self.forward if direction > 0 else self.backward


def tie_kernel(*refs):
    pass


def tie(x, *after):
    return pl.pallas_call(
        tie_kernel,
        out_shape=jax.ShapeDtypeStruct(x.shape, x.dtype),
        in_specs=[ANY] * (1 + len(after)),
        out_specs=ANY,
        input_output_aliases={0: 0},
        name="tie",
    )(x, *after)


def gather_ring(plan, chunk, after=None, during=None):
    pieces = [[chunk[lo:hi]] for _, lo, hi in plan.streams]
    heads_of = [stream[0] for stream in pieces]
    if after is not None:
        heads_of = [tie(x, after[k]) for k, x in enumerate(heads_of)]
    for step in range(1, plan.n_owners):
        for k, (direction, _, _) in enumerate(plan.streams):
            last = heads_of[k] if step == 1 else pieces[k][step - 1]
            if during and k == 0 and step in during:
                last = tie(last, *during[step])
            pieces[k].append(lax.ppermute(last, "fsdp", plan.perm(direction)))
    return pieces


def reduce_ring(plan, pieces, factor):
    n = plan.n_owners
    held = [pieces[k][1] for k in range(len(plan.streams))]
    for step in range(2, n + 1):
        for k, (direction, _, _) in enumerate(plan.streams):
            arrived = lax.ppermute(held[k], "fsdp", plan.perm(direction))
            own = pieces[k][step % n]
            if step < n:
                held[k] = arrived + own
            else:
                held[k] = (arrived.astype(F32) + own.astype(F32)) * factor
    return jnp.concatenate(held, axis=0)


def swap(x, bit, n):
    return lax.ppermute(x, "seq", [(i, i ^ bit) for i in range(n)])


def reduce_columns(parts, n):
    parts = dict(enumerate(parts))
    bit = 1
    while 2 * bit < n:
        for r in [r for r in parts if r & bit]:
            parts[r ^ bit] = parts[r ^ bit] + swap(parts.pop(r), bit, n)
        bit *= 2
    return parts[0], swap(parts[bit], bit, n)


def gather_columns(share, n):
    parts = {0: share}
    bit = n // 2
    while bit:
        for r in list(parts):
            parts[r ^ bit] = swap(parts[r], bit, n)
        bit //= 2
    return [parts[r] for r in range(n)]


def loop_blocks(plan, table, k, step, lo, hi, on_qkv, on_out):
    row = 0 if plan.streams[k][0] > 0 else 2
    start, count = table[row, step], table[row + 1, step]
    end = jnp.clip(count, lo, hi)
    middle = jnp.clip(plan.split - start, lo, end)

    def sweep(first, last, block, cols, visit):
        def one(t, at):
            r, c = at
            visit(t - lo, r, c)
            wrap = c + 1 == cols
            return jnp.where(wrap, r + 1, r), jnp.where(wrap, 0, c + 1)

        lax.fori_loop(first, last, one, (lax.div(block, cols), lax.rem(block, cols)))

    sweep(lo, middle, start + lo, plan.qkv_cols, on_qkv)
    sweep(middle, end, start + middle - plan.split, plan.d_blocks, on_out)


def tile(ref, row, col):
    return ref.at[
        pl.ds(pl.multiple_of(row * BLK, BLK), BLK), pl.ds(pl.multiple_of(col * BLK, BLK), BLK)
    ]


def unpack(plan, table, refs, qkv, out, qkv_sem, out_sem):
    at = 0
    for k, (_, lo, hi) in enumerate(plan.streams):
        for step in range(plan.n_owners):
            ref = refs[at]
            at += 1
            loop_blocks(
                plan, table, k, step, lo, hi,
                lambda t, r, c, ref=ref: pltpu.make_async_copy(ref.at[t], tile(qkv, r, c), qkv_sem).start(),
                lambda t, r, c, ref=ref: pltpu.make_async_copy(ref.at[t], tile(out, r, c), out_sem).start(),
            )


def wait_all(ref, sem):
    pltpu.make_async_copy(ref, ref, sem).wait()


def turn(x, cosine, sine):
    return x * cosine + pltpu.roll(x, HD // 2, 1) * sine


def softmax_rows(plan, q, keys, first, end):
    scores = dot_nt(q, keys) * HD ** (-0.5)
    rows = lax.broadcasted_iota(jnp.int32, scores.shape, 0) + first
    cols = lax.broadcasted_iota(jnp.int32, scores.shape, 1)
    scores = jnp.where(rows >= cols, scores, NEGATIVE)
    scores = jnp.exp(scores - jnp.max(scores, axis=1, keepdims=True))
    return scores / jnp.sum(scores, axis=1, keepdims=True)


def each_head(plan, visit):
    def columns(at):
        return pl.ds(pl.multiple_of(at, HD), HD)

    def one(head, carry):
        kv = lax.div(head, plan.group)
        visit(
            columns(head * HD), columns(plan.q_end + kv * HD), columns(plan.k_end + kv * HD), kv
        )
        return carry

    lax.fori_loop(0, plan.q_heads, one, 0)


def row_blocks(plan):
    return [(first, first + plan.rows) for first in range(0, plan.length, plan.rows)]


def project(plan, normed, matrix, result):
    cosine, sine, sink = result[1], result[2], result[0]
    step = 2 * HD
    for first in range(0, plan.width, step):
        end = min(first + step, plan.width)
        part = dot(normed[...], matrix[:, first:end])
        for at in range(first, end, HD):
            piece = part[:, at - first : at - first + HD]
            if at < plan.k_end:
                piece = turn(piece, cosine[...], sine[...])
            sink[:, at : at + HD] = piece.astype(BF16)


def weight_kernel(plan, table, normed, cosine, sine, *rest):
    n_refs = len(plan.streams) * plan.n_owners
    refs = rest[:n_refs]
    fields, w_out, w_qkv, qkv_sem, out_sem = rest[n_refs:]
    unpack(plan, table, refs, w_qkv, w_out, qkv_sem, out_sem)
    wait_all(w_qkv, qkv_sem)
    project(plan, normed, w_qkv, (fields, cosine, sine))
    wait_all(w_out, out_sem)


def mix_kernel(plan, fields, mixed):
    def visit(q_at, k_at, v_at, kv):
        for first, end in row_blocks(plan):
            probs = softmax_rows(plan, fields[first:end, q_at], fields[:end, k_at], first, end)
            mixed[first:end, q_at] = dot(probs.astype(BF16), fields[:end, v_at]).astype(BF16)

    each_head(plan, visit)


def probe_kernel(plan, shares, table, cosine, sine, fields, normed_hbm, mixed_hbm, w_out_hbm, *rest):
    n_refs = len(plan.streams) * plan.n_owners
    refs = rest[:n_refs]
    ends = row_blocks(plan)
    n_out = shares * len(ends)
    sinks = rest[n_refs : n_refs + n_out]
    p_qkv, both_out, moved, both_mixed, normed, tangents, qkv_sem, out_sem, sems, sink_sems = rest[n_refs + n_out :]
    copies = [
        pltpu.make_async_copy(normed_hbm, normed, sems.at[0]),
        pltpu.make_async_copy(mixed_hbm, both_mixed.at[:, pl.ds(plan.q_end, plan.q_end)], sems.at[1]),
        pltpu.make_async_copy(w_out_hbm, both_out.at[pl.ds(0, plan.q_end), :], sems.at[2]),
    ]
    for copy in copies:
        copy.start()
    p_out = both_out.at[pl.ds(plan.q_end, plan.q_end), :]
    mixed_moved = both_mixed
    unpack(plan, table, refs, p_qkv, p_out, qkv_sem, out_sem)
    copies[0].wait()
    wait_all(p_qkv, qkv_sem)
    project(plan, normed, p_qkv, (moved, cosine, sine))

    def visit(q_at, k_at, v_at, kv):
        for first, end in row_blocks(plan):
            q, dq = fields[first:end, q_at], moved[first:end, q_at]
            keys, d_keys = fields[:end, k_at], moved[:end, k_at]
            values, d_values = fields[:end, v_at], moved[:end, v_at]
            probs = softmax_rows(plan, q, keys, first, end)
            d_scores = (dot_nt(dq, keys) + dot_nt(q, d_keys)) * HD ** (-0.5)
            d_probs = probs * (d_scores - jnp.sum(probs * d_scores, axis=1, keepdims=True))
            mixed_moved[first:end, q_at] = (
                dot(d_probs.astype(BF16), values) + dot(probs.astype(BF16), d_values)
            ).astype(BF16)

    each_head(plan, visit)
    copies[1].wait()
    copies[2].wait()
    wait_all(p_out, out_sem)
    step = 2 * BLK
    share = D // shares
    done = []
    for r in range(shares):
        base = (table[4, 0] ^ r) * share

        def columns(i, carry, r=r, base=base):
            here = pl.ds(pl.multiple_of(i * step, step), step)
            there = pl.ds(pl.multiple_of(base + i * step, step), step)
            part = dot(both_mixed[...], both_out[:, there])
            for j, (first, end) in enumerate(ends):
                tangents[j * shares + r, :, here] = part[first:end].astype(BF16)
            return carry

        lax.fori_loop(0, share // step, columns, 0)
        for j in range(len(ends)):
            at = j * shares + r
            done.append(pltpu.make_async_copy(tangents.at[at], sinks[at], sink_sems.at[at]))
            done[-1].start()
    for copy in done:
        copy.wait()


def pull_kernel(plan, shares, table, normed_t_hbm, w_out, fields, mixed_t, cosine, sine, *rest):
    ends = row_blocks(plan)
    weighted = rest[: shares * len(ends)]
    n_refs = len(plan.streams) * plan.n_owners
    refs = rest[len(weighted) : len(weighted) + n_refs]
    g_qkv, g_out, d_mixed, d_proj, normed_t, d_keys, d_values, qkv_sem, out_sem, sem = rest[len(weighted) + n_refs :]
    copy = pltpu.make_async_copy(normed_t_hbm, normed_t, sem)
    copy.start()
    step = 2 * BLK
    share = D // shares
    total = [None] * len(ends)
    for r in range(shares):
        base = (table[4, 0] ^ r) * share
        for j, (first, end) in enumerate(ends):
            part = dot_nt(weighted[j * shares + r][...], w_out[:, pl.ds(pl.multiple_of(base, share), share)])
            total[j] = part if total[j] is None else total[j] + part
    for j, (first, end) in enumerate(ends):
        d_mixed[first:end, :] = total[j].astype(BF16)
    for r in range(shares):
        base = (table[4, 0] ^ r) * share

        def columns(i, carry, r=r, base=base):
            here = pl.ds(pl.multiple_of(i * step, step), step)
            there = pl.ds(pl.multiple_of(base + i * step, step), step)
            part = None
            for j, (first, end) in enumerate(ends):
                more = dot(mixed_t[:, first:end], weighted[j * shares + r][:, here])
                part = more if part is None else part + more
            g_out[:, there] = part.astype(BF16)
            return carry

        lax.fori_loop(0, share // step, columns, 0)
    scale = HD ** (-0.5)
    d_keys[...] = jnp.zeros_like(d_keys)
    d_values[...] = jnp.zeros_like(d_values)

    def visit(q_at, k_at, v_at, kv):
        kv_at = pl.ds(pl.multiple_of(kv * HD, HD), HD)
        for first, end in ends:
            q, d_mix = fields[first:end, q_at], d_mixed[first:end, q_at]
            keys, values = fields[:end, k_at], fields[:end, v_at]
            probs = softmax_rows(plan, q, keys, first, end)
            d_probs = dot_nt(d_mix, values).astype(BF16).astype(F32)
            d_scores = probs * (d_probs - jnp.sum(probs * d_probs, axis=1, keepdims=True))
            d_scores = (d_scores * scale).astype(BF16)
            d_q = dot(d_scores, keys).astype(BF16).astype(F32)
            d_proj[first:end, q_at] = turn(
                d_q, cosine[first:end, :], -sine[first:end, :]
            ).astype(BF16)
            d_keys[:end, kv_at] += dot_tn(d_scores, q)
            d_values[:end, kv_at] += dot_tn(probs.astype(BF16), d_mix)

    each_head(plan, visit)
    for kv in range(plan.kv_heads):
        at = slice(kv * HD, (kv + 1) * HD)
        d_proj[:, plan.q_end + kv * HD : plan.q_end + (kv + 1) * HD] = turn(
            d_keys[:, at].astype(BF16).astype(F32), cosine[...], -sine[...]
        ).astype(BF16)
        d_proj[:, plan.k_end + kv * HD : plan.k_end + (kv + 1) * HD] = d_values[:, at].astype(BF16)
    copy.wait()
    rows = 4 * BLK

    def qkv_rows(i, carry):
        at = pl.ds(pl.multiple_of(i * rows, rows), rows)
        g_qkv[at, :] = dot(normed_t[at, :], d_proj[...]).astype(BF16)
        return carry

    lax.fori_loop(0, D // rows, qkv_rows, 0)
    at = 0
    for k, (_, lo, hi) in enumerate(plan.streams):
        for step in range(plan.n_owners):
            ref = refs[at]
            at += 1
            loop_blocks(
                plan, table, k, step, lo, hi,
                lambda t, r, c, ref=ref: pltpu.make_async_copy(tile(g_qkv, r, c), ref.at[t], qkv_sem).start(),
                lambda t, r, c, ref=ref: pltpu.make_async_copy(tile(g_out, r, c), ref.at[t], out_sem).start(),
            )
    wait_all(g_qkv, qkv_sem)
    wait_all(g_out, out_sem)


VMEM = pl.BlockSpec(memory_space=pltpu.VMEM)
SMEM = pl.BlockSpec(memory_space=pltpu.SMEM)
ANY = pl.BlockSpec(memory_space=pl.ANY)
HBM = pl.BlockSpec(memory_space=pltpu.HBM)
PARAMS = pltpu.CompilerParams(vmem_limit_bytes=58 * 1024 * 1024)


def flat(pieces):
    return [piece for stream in pieces for piece in stream]


def local(tokens, norm_gain, curvature, weight_slots, probe_slots, block_counts):
    n_columns = lax.axis_size("seq")
    n_owners = lax.axis_size("fsdp")
    slots = weight_slots.shape[1]
    length = tokens.shape[1]
    plan = Plan(length, slots, n_columns, n_owners)
    counts = block_counts[0]
    range_ends = jnp.cumsum(counts)
    starts = range_ends - counts
    me = lax.axis_index("fsdp")
    column = lax.axis_index("seq")
    order = jnp.array(plan.order, jnp.int32)
    owner_ids = jnp.arange(n_owners, dtype=jnp.int32)
    place = jnp.sum(jnp.where(order == me, owner_ids, 0))
    behind = order[(place - owner_ids) % n_owners]
    ahead = order[(place + owner_ids) % n_owners]
    own_column = jnp.full((n_owners,), column, jnp.int32)
    table = jnp.stack(
        [starts[behind], counts[behind], starts[ahead], counts[ahead], own_column]
    ).astype(jnp.int32)

    n = n_owners
    w_pieces = gather_ring(plan, weight_slots[0])
    values = tokens[0].astype(F32)
    factor = lax.rsqrt(jnp.mean(values * values, axis=-1, keepdims=True) + EPS)
    normed = (values * factor * norm_gain).astype(BF16)
    cosine, sine = rotary(length, HD)
    sem = pltpu.SemaphoreType.DMA
    halves = len(row_blocks(plan))
    share = D // n_columns

    n_refs = len(plan.streams) * n
    fields, w_out = pl.pallas_call(
        lambda *refs: weight_kernel(plan, *refs),
        out_shape=[
            jax.ShapeDtypeStruct((length, plan.width), BF16),
            jax.ShapeDtypeStruct((plan.q_end, D), BF16),
        ],
        in_specs=[SMEM] + [VMEM] * 3 + [ANY] * n_refs,
        out_specs=[VMEM] * 2,
        scratch_shapes=[pltpu.VMEM((D, plan.width), BF16), sem, sem],
        compiler_params=PARAMS,
        name="weights",
    )(table, normed, cosine, sine, *flat(w_pieces))
    mixed = pl.pallas_call(
        lambda *refs: mix_kernel(plan, *refs),
        out_shape=jax.ShapeDtypeStruct((length, plan.q_end), BF16),
        in_specs=[VMEM],
        out_specs=VMEM,
        compiler_params=PARAMS,
        name="mix",
    )(fields)
    normed_t, mixed_t = normed.T, mixed.T
    p_pieces = gather_ring(
        plan,
        probe_slots[0],
        [stream[n - 2] for stream in w_pieces],
        {2: (fields,), 4: (mixed,), 5: (normed_t, mixed_t)},
    )
    tangents = pl.pallas_call(
        lambda *refs: probe_kernel(plan, n_columns, *refs),
        out_shape=[jax.ShapeDtypeStruct((plan.rows, share), BF16)] * (halves * n_columns),
        in_specs=[SMEM] + [VMEM] * 3 + [HBM] * 3 + [ANY] * n_refs,
        out_specs=[HBM] * (halves * n_columns),
        scratch_shapes=[
            pltpu.VMEM((D, plan.width), BF16),
            pltpu.VMEM((2 * plan.q_end, D), BF16),
            pltpu.VMEM((length, plan.width), BF16),
            pltpu.VMEM((length, 2 * plan.q_end), BF16),
            pltpu.VMEM((length, D), BF16),
            pltpu.VMEM((halves * n_columns, plan.rows, share), BF16),
            sem,
            sem,
            pltpu.SemaphoreType.DMA((3,)),
            pltpu.SemaphoreType.DMA((halves * n_columns,)),
        ],
        compiler_params=PARAMS,
        name="probe",
    )(table, cosine, sine, fields, normed, mixed, w_out, *flat(p_pieces))
    curv_share = lax.dynamic_slice_in_dim(curvature[0], column * share, share, 1)
    weighted = []
    for j, (first, end) in enumerate(row_blocks(plan)):
        own, other = reduce_columns(tangents[j * n_columns : (j + 1) * n_columns], n_columns)
        total = own.astype(F32) + other.astype(F32)
        mine = (curv_share[first:end].astype(F32) * total).astype(BF16)
        weighted += gather_columns(mine, n_columns)

    pieces = pl.pallas_call(
        lambda *refs: pull_kernel(plan, n_columns, *refs),
        out_shape=[
            jax.ShapeDtypeStruct((hi - lo, BLK, BLK), BF16)
            for _, lo, hi in plan.streams
            for _ in range(n)
        ],
        in_specs=[SMEM, HBM] + [VMEM] * (5 + halves * n_columns),
        out_specs=[ANY] * n_refs,
        scratch_shapes=[
            pltpu.VMEM((D, plan.width), BF16),
            pltpu.VMEM((plan.q_end, D), BF16),
            pltpu.VMEM((length, plan.q_end), BF16),
            pltpu.VMEM((length, plan.width), BF16),
            pltpu.VMEM((D, length), BF16),
            pltpu.VMEM((length, plan.kv_heads * HD), F32),
            pltpu.VMEM((length, plan.kv_heads * HD), F32),
            sem,
            sem,
            sem,
        ],
        compiler_params=PARAMS,
        name="pull",
    )(table, normed_t, w_out, fields, mixed_t, cosine, sine, *weighted)

    pieces = [pieces[k * n : (k + 1) * n] for k in range(len(plan.streams))]
    summed = reduce_ring(plan, pieces, 1.0 / jnp.sqrt(F32(length * n_owners)))
    live = jnp.arange(slots, dtype=jnp.int32) < counts[me]
    return jnp.where(live[:, None, None], summed, 0.0)[None]


def solution(mesh):
    in_specs = (
        P("fsdp", None, None),
        P(),
        P("fsdp", None, None),
        P("seq", "fsdp", None, None),
        P("seq", "fsdp", None, None),
        P("seq", None),
    )
    out_specs = P("seq", "fsdp", None, None)
    return jax.shard_map(local, mesh=mesh, in_specs=in_specs, out_specs=out_specs, check_vma=False)
```

```python
import jax
import jax.numpy as jnp
from jax import lax
from jax.experimental import pallas as pl
from jax.experimental.pallas import tpu as pltpu
from jax.sharding import PartitionSpec as P

D = 4096
HQ = 16
HK = 4
HD = 128
BLK = 128

THETA = 500000.0
EPS = 1e-05
NEGATIVE = -1e30

STREAMS = 4
F32 = jnp.float32
BF16 = jnp.bfloat16


def rotary(length, head_dim):
    half_dim = head_dim // 2
    frequency = jnp.exp(-jnp.log(THETA) * 2.0 * jnp.arange(half_dim, dtype=F32) / head_dim)
    angles = jnp.arange(length, dtype=F32)[:, None] * frequency[None, :]
    cosine, sine = jnp.cos(angles), jnp.sin(angles)
    return jnp.concatenate([cosine, cosine], axis=1), jnp.concatenate([-sine, sine], axis=1)


def dot(a, b):
    return jnp.dot(a, b, preferred_element_type=F32)


def dot_nt(a, b):
    return lax.dot_general(a, b, (((1,), (1,)), ((), ())), preferred_element_type=F32)


def dot_tn(a, b):
    return lax.dot_general(a, b, (((0,), (0,)), ((), ())), preferred_element_type=F32)


class Plan:
    def __init__(self, length, slots, n_columns, n_owners):
        self.length, self.slots = length, slots
        self.n_owners = n_owners
        self.q_heads = HQ // n_columns
        self.kv_heads = HK // n_columns
        self.group = self.q_heads // self.kv_heads
        self.q_end = self.q_heads * HD
        self.k_end = self.q_end + self.kv_heads * HD
        self.width = self.k_end + self.kv_heads * HD
        self.qkv_cols = self.width // BLK
        self.d_blocks = D // BLK
        self.split = self.d_blocks * self.qkv_cols
        self.total = self.split + self.q_end // BLK * self.d_blocks
        self.rows = min(256, length)
        evens = list(range(0, n_owners, 2))
        odds = list(range(1, n_owners, 2))[::-1]
        self.order = evens + odds
        cuts = [slots * k // STREAMS for k in range(STREAMS + 1)]
        self.streams = [
            (1 if k < STREAMS // 2 else -1, cuts[k], cuts[k + 1]) for k in range(STREAMS)
        ]
        n = n_owners
        self.forward = [(self.order[i], self.order[(i + 1) % n]) for i in range(n)]
        self.backward = [(b, a) for a, b in self.forward]

    def perm(self, direction):
        return self.forward if direction > 0 else self.backward


def tie_kernel(*refs):
    pass


def tie(x, *after):
    return pl.pallas_call(
        tie_kernel,
        out_shape=jax.ShapeDtypeStruct(x.shape, x.dtype),
        in_specs=[ANY] * (1 + len(after)),
        out_specs=ANY,
        input_output_aliases={0: 0},
        name="tie",
    )(x, *after)


def gather_ring(plan, chunk, after=None, during=None):
    pieces = [[chunk[lo:hi]] for _, lo, hi in plan.streams]
    heads_of = [stream[0] for stream in pieces]
    if after is not None:
        heads_of = [tie(x, after[k]) for k, x in enumerate(heads_of)]
    for step in range(1, plan.n_owners):
        for k, (direction, _, _) in enumerate(plan.streams):
            last = heads_of[k] if step == 1 else pieces[k][step - 1]
            if during and k == 0 and step in during:
                last = tie(last, *during[step])
            pieces[k].append(lax.ppermute(last, "fsdp", plan.perm(direction)))
    return pieces


def reduce_ring(plan, pieces, factor):
    n = plan.n_owners
    held = [pieces[k][1] for k in range(len(plan.streams))]
    for step in range(2, n + 1):
        for k, (direction, _, _) in enumerate(plan.streams):
            arrived = lax.ppermute(held[k], "fsdp", plan.perm(direction))
            own = pieces[k][step % n]
            if step < n:
                held[k] = arrived + own
            else:
                held[k] = (arrived.astype(F32) + own.astype(F32)) * factor
    return jnp.concatenate(held, axis=0)


def swap(x, bit, n):
    return lax.ppermute(x, "seq", [(i, i ^ bit) for i in range(n)])


def reduce_columns(parts, n):
    parts = dict(enumerate(parts))
    bit = 1
    while 2 * bit < n:
        for r in [r for r in parts if r & bit]:
            parts[r ^ bit] = parts[r ^ bit] + swap(parts.pop(r), bit, n)
        bit *= 2
    return parts[0], swap(parts[bit], bit, n)


def gather_columns(share, n):
    parts = {0: share}
    bit = n // 2
    while bit:
        for r in list(parts):
            parts[r ^ bit] = swap(parts[r], bit, n)
        bit //= 2
    return [parts[r] for r in range(n)]


def loop_blocks(plan, table, k, step, lo, hi, on_qkv, on_out):
    row = 0 if plan.streams[k][0] > 0 else 2
    start, count = table[row, step], table[row + 1, step]
    end = jnp.clip(count, lo, hi)
    middle = jnp.clip(plan.split - start, lo, end)

    def sweep(first, last, block, cols, visit):
        def one(t, at):
            r, c = at
            visit(t - lo, r, c)
            wrap = c + 1 == cols
            return jnp.where(wrap, r + 1, r), jnp.where(wrap, 0, c + 1)

        lax.fori_loop(first, last, one, (lax.div(block, cols), lax.rem(block, cols)))

    sweep(lo, middle, start + lo, plan.qkv_cols, on_qkv)
    sweep(middle, end, start + middle - plan.split, plan.d_blocks, on_out)


def tile(ref, row, col):
    return ref.at[
        pl.ds(pl.multiple_of(row * BLK, BLK), BLK), pl.ds(pl.multiple_of(col * BLK, BLK), BLK)
    ]


def unpack(plan, table, refs, qkv, out, qkv_sem, out_sem):
    at = 0
    for k, (_, lo, hi) in enumerate(plan.streams):
        for step in range(plan.n_owners):
            ref = refs[at]
            at += 1
            loop_blocks(
                plan, table, k, step, lo, hi,
                lambda t, r, c, ref=ref: pltpu.make_async_copy(ref.at[t], tile(qkv, r, c), qkv_sem).start(),
                lambda t, r, c, ref=ref: pltpu.make_async_copy(ref.at[t], tile(out, r, c), out_sem).start(),
            )


def wait_all(ref, sem):
    pltpu.make_async_copy(ref, ref, sem).wait()


def turn(x, cosine, sine):
    return x * cosine + pltpu.roll(x, HD // 2, 1) * sine


def softmax_rows(plan, q, keys, first, end):
    scores = dot_nt(q, keys) * HD ** (-0.5)
    rows = lax.broadcasted_iota(jnp.int32, scores.shape, 0) + first
    cols = lax.broadcasted_iota(jnp.int32, scores.shape, 1)
    scores = jnp.where(rows >= cols, scores, NEGATIVE)
    scores = jnp.exp(scores - jnp.max(scores, axis=1, keepdims=True))
    return scores / jnp.sum(scores, axis=1, keepdims=True)


def each_head(plan, visit):
    def columns(at):
        return pl.ds(pl.multiple_of(at, HD), HD)

    def one(head, carry):
        kv = lax.div(head, plan.group)
        visit(
            columns(head * HD), columns(plan.q_end + kv * HD), columns(plan.k_end + kv * HD), kv
        )
        return carry

    lax.fori_loop(0, plan.q_heads, one, 0)


def row_blocks(plan):
    return [(first, first + plan.rows) for first in range(0, plan.length, plan.rows)]


def project(plan, normed, matrix, result):
    cosine, sine, sink = result[1], result[2], result[0]
    step = 2 * HD
    for first in range(0, plan.width, step):
        end = min(first + step, plan.width)
        part = dot(normed[...], matrix[:, first:end])
        for at in range(first, end, HD):
            piece = part[:, at - first : at - first + HD]
            if at < plan.k_end:
                piece = turn(piece, cosine[...], sine[...])
            sink[:, at : at + HD] = piece.astype(BF16)


def weight_kernel(plan, table, cosine, sine, normed_hbm, *rest):
    n_refs = len(plan.streams) * plan.n_owners
    refs = rest[:n_refs]
    fields, w_out_hbm, w_qkv, w_out, normed, qkv_sem, out_sem, sems = rest[n_refs:]
    arrive = pltpu.make_async_copy(normed_hbm, normed, sems.at[0])
    leave = pltpu.make_async_copy(w_out, w_out_hbm, sems.at[1])
    arrive.start()
    unpack(plan, table, refs, w_qkv, w_out, qkv_sem, out_sem)
    arrive.wait()
    wait_all(w_qkv, qkv_sem)
    wait_all(w_out, out_sem)
    leave.start()
    project(plan, normed, w_qkv, (fields, cosine, sine))
    leave.wait()


def mix_kernel(plan, fields, mixed):
    def visit(q_at, k_at, v_at, kv):
        for first, end in row_blocks(plan):
            probs = softmax_rows(plan, fields[first:end, q_at], fields[:end, k_at], first, end)
            mixed[first:end, q_at] = dot(probs.astype(BF16), fields[:end, v_at]).astype(BF16)

    each_head(plan, visit)


def probe_kernel(plan, shares, table, cosine, sine, fields, normed_hbm, mixed_hbm, w_out_hbm, *rest):
    n_refs = len(plan.streams) * plan.n_owners
    refs = rest[:n_refs]
    ends = row_blocks(plan)
    n_out = shares * len(ends)
    sinks = rest[n_refs : n_refs + n_out]
    p_qkv, both_out, moved, both_mixed, normed, tangents, qkv_sem, out_sem, sems, sink_sems = rest[n_refs + n_out :]
    copies = [
        pltpu.make_async_copy(normed_hbm, normed, sems.at[0]),
        pltpu.make_async_copy(mixed_hbm, both_mixed.at[:, pl.ds(plan.q_end, plan.q_end)], sems.at[1]),
        pltpu.make_async_copy(w_out_hbm, both_out.at[pl.ds(0, plan.q_end), :], sems.at[2]),
    ]
    for copy in copies:
        copy.start()
    p_out = both_out.at[pl.ds(plan.q_end, plan.q_end), :]
    mixed_moved = both_mixed
    unpack(plan, table, refs, p_qkv, p_out, qkv_sem, out_sem)
    copies[0].wait()
    wait_all(p_qkv, qkv_sem)
    project(plan, normed, p_qkv, (moved, cosine, sine))

    def visit(q_at, k_at, v_at, kv):
        for first, end in row_blocks(plan):
            q, dq = fields[first:end, q_at], moved[first:end, q_at]
            keys, d_keys = fields[:end, k_at], moved[:end, k_at]
            values, d_values = fields[:end, v_at], moved[:end, v_at]
            probs = softmax_rows(plan, q, keys, first, end)
            d_scores = (dot_nt(dq, keys) + dot_nt(q, d_keys)) * HD ** (-0.5)
            d_probs = probs * (d_scores - jnp.sum(probs * d_scores, axis=1, keepdims=True))
            mixed_moved[first:end, q_at] = (
                dot(d_probs.astype(BF16), values) + dot(probs.astype(BF16), d_values)
            ).astype(BF16)

    each_head(plan, visit)
    copies[1].wait()
    copies[2].wait()
    wait_all(p_out, out_sem)
    step = 2 * BLK
    share = D // shares
    done = []
    for r in range(shares):
        base = (table[4, 0] ^ r) * share

        def columns(i, carry, r=r, base=base):
            here = pl.ds(pl.multiple_of(i * step, step), step)
            there = pl.ds(pl.multiple_of(base + i * step, step), step)
            part = dot(both_mixed[...], both_out[:, there])
            for j, (first, end) in enumerate(ends):
                tangents[j * shares + r, :, here] = part[first:end].astype(BF16)
            return carry

        lax.fori_loop(0, share // step, columns, 0)
        for j in range(len(ends)):
            at = j * shares + r
            done.append(pltpu.make_async_copy(tangents.at[at], sinks[at], sink_sems.at[at]))
            done[-1].start()
    for copy in done:
        copy.wait()


def pull_kernel(plan, shares, table, normed_t_hbm, w_out, fields, mixed_t, cosine, sine, *rest):
    ends = row_blocks(plan)
    weighted = rest[: shares * len(ends)]
    n_refs = len(plan.streams) * plan.n_owners
    refs = rest[len(weighted) : len(weighted) + n_refs]
    g_qkv, g_out, d_mixed, d_proj, normed_t, d_keys, d_values, qkv_sem, out_sem, sem = rest[len(weighted) + n_refs :]
    copy = pltpu.make_async_copy(normed_t_hbm, normed_t, sem)
    copy.start()
    step = 2 * BLK
    share = D // shares
    total = [None] * len(ends)
    for r in range(shares):
        base = (table[4, 0] ^ r) * share
        for j, (first, end) in enumerate(ends):
            part = dot_nt(weighted[j * shares + r][...], w_out[:, pl.ds(pl.multiple_of(base, share), share)])
            total[j] = part if total[j] is None else total[j] + part
    for j, (first, end) in enumerate(ends):
        d_mixed[first:end, :] = total[j].astype(BF16)
    for r in range(shares):
        base = (table[4, 0] ^ r) * share

        def columns(i, carry, r=r, base=base):
            here = pl.ds(pl.multiple_of(i * step, step), step)
            there = pl.ds(pl.multiple_of(base + i * step, step), step)
            part = None
            for j, (first, end) in enumerate(ends):
                more = dot(mixed_t[:, first:end], weighted[j * shares + r][:, here])
                part = more if part is None else part + more
            g_out[:, there] = part.astype(BF16)
            return carry

        lax.fori_loop(0, share // step, columns, 0)
    scale = HD ** (-0.5)
    d_keys[...] = jnp.zeros_like(d_keys)
    d_values[...] = jnp.zeros_like(d_values)

    def visit(q_at, k_at, v_at, kv):
        kv_at = pl.ds(pl.multiple_of(kv * HD, HD), HD)
        for first, end in ends:
            q, d_mix = fields[first:end, q_at], d_mixed[first:end, q_at]
            keys, values = fields[:end, k_at], fields[:end, v_at]
            probs = softmax_rows(plan, q, keys, first, end)
            d_probs = dot_nt(d_mix, values).astype(BF16).astype(F32)
            d_scores = probs * (d_probs - jnp.sum(probs * d_probs, axis=1, keepdims=True))
            d_scores = (d_scores * scale).astype(BF16)
            d_q = dot(d_scores, keys).astype(BF16).astype(F32)
            d_proj[first:end, q_at] = turn(
                d_q, cosine[first:end, :], -sine[first:end, :]
            ).astype(BF16)
            d_keys[:end, kv_at] += dot_tn(d_scores, q)
            d_values[:end, kv_at] += dot_tn(probs.astype(BF16), d_mix)

    each_head(plan, visit)
    for kv in range(plan.kv_heads):
        at = slice(kv * HD, (kv + 1) * HD)
        d_proj[:, plan.q_end + kv * HD : plan.q_end + (kv + 1) * HD] = turn(
            d_keys[:, at].astype(BF16).astype(F32), cosine[...], -sine[...]
        ).astype(BF16)
        d_proj[:, plan.k_end + kv * HD : plan.k_end + (kv + 1) * HD] = d_values[:, at].astype(BF16)
    copy.wait()
    rows = 4 * BLK

    def qkv_rows(i, carry):
        at = pl.ds(pl.multiple_of(i * rows, rows), rows)
        g_qkv[at, :] = dot(normed_t[at, :], d_proj[...]).astype(BF16)
        return carry

    lax.fori_loop(0, D // rows, qkv_rows, 0)
    at = 0
    for k, (_, lo, hi) in enumerate(plan.streams):
        for step in range(plan.n_owners):
            ref = refs[at]
            at += 1
            loop_blocks(
                plan, table, k, step, lo, hi,
                lambda t, r, c, ref=ref: pltpu.make_async_copy(tile(g_qkv, r, c), ref.at[t], qkv_sem).start(),
                lambda t, r, c, ref=ref: pltpu.make_async_copy(tile(g_out, r, c), ref.at[t], out_sem).start(),
            )
    wait_all(g_qkv, qkv_sem)
    wait_all(g_out, out_sem)


VMEM = pl.BlockSpec(memory_space=pltpu.VMEM)
SMEM = pl.BlockSpec(memory_space=pltpu.SMEM)
ANY = pl.BlockSpec(memory_space=pl.ANY)
HBM = pl.BlockSpec(memory_space=pltpu.HBM)
PARAMS = pltpu.CompilerParams(vmem_limit_bytes=58 * 1024 * 1024)


def flat(pieces):
    return [piece for stream in pieces for piece in stream]


def local(tokens, norm_gain, curvature, weight_slots, probe_slots, block_counts):
    n_columns = lax.axis_size("seq")
    n_owners = lax.axis_size("fsdp")
    slots = weight_slots.shape[1]
    length = tokens.shape[1]
    plan = Plan(length, slots, n_columns, n_owners)
    counts = block_counts[0]
    range_ends = jnp.cumsum(counts)
    starts = range_ends - counts
    me = lax.axis_index("fsdp")
    column = lax.axis_index("seq")
    order = jnp.array(plan.order, jnp.int32)
    owner_ids = jnp.arange(n_owners, dtype=jnp.int32)
    place = jnp.sum(jnp.where(order == me, owner_ids, 0))
    behind = order[(place - owner_ids) % n_owners]
    ahead = order[(place + owner_ids) % n_owners]
    own_column = jnp.full((n_owners,), column, jnp.int32)
    table = jnp.stack(
        [starts[behind], counts[behind], starts[ahead], counts[ahead], own_column]
    ).astype(jnp.int32)

    n = n_owners
    w_pieces = gather_ring(plan, weight_slots[0])
    values = tokens[0].astype(F32)
    factor = lax.rsqrt(jnp.mean(values * values, axis=-1, keepdims=True) + EPS)
    normed = (values * factor * norm_gain).astype(BF16)
    cosine, sine = rotary(length, HD)
    sem = pltpu.SemaphoreType.DMA
    halves = len(row_blocks(plan))
    share = D // n_columns

    n_refs = len(plan.streams) * n
    fields, w_out = pl.pallas_call(
        lambda *refs: weight_kernel(plan, *refs),
        out_shape=[
            jax.ShapeDtypeStruct((length, plan.width), BF16),
            jax.ShapeDtypeStruct((plan.q_end, D), BF16),
        ],
        in_specs=[SMEM] + [VMEM] * 2 + [HBM] + [ANY] * n_refs,
        out_specs=[VMEM, HBM],
        scratch_shapes=[
            pltpu.VMEM((D, plan.width), BF16),
            pltpu.VMEM((plan.q_end, D), BF16),
            pltpu.VMEM((length, D), BF16),
            sem,
            sem,
            pltpu.SemaphoreType.DMA((2,)),
        ],
        compiler_params=PARAMS,
        name="weights",
    )(table, cosine, sine, normed, *flat(w_pieces))
    mixed = pl.pallas_call(
        lambda *refs: mix_kernel(plan, *refs),
        out_shape=jax.ShapeDtypeStruct((length, plan.q_end), BF16),
        in_specs=[VMEM],
        out_specs=VMEM,
        compiler_params=PARAMS,
        name="mix",
    )(fields)
    normed_t, mixed_t = normed.T, mixed.T
    p_pieces = gather_ring(
        plan,
        probe_slots[0],
        [stream[n - 2] for stream in w_pieces],
        {2: (fields,), 4: (mixed,), 5: (normed_t, mixed_t)},
    )
    tangents = pl.pallas_call(
        lambda *refs: probe_kernel(plan, n_columns, *refs),
        out_shape=[jax.ShapeDtypeStruct((plan.rows, share), BF16)] * (halves * n_columns),
        in_specs=[SMEM] + [VMEM] * 3 + [HBM] * 3 + [ANY] * n_refs,
        out_specs=[HBM] * (halves * n_columns),
        scratch_shapes=[
            pltpu.VMEM((D, plan.width), BF16),
            pltpu.VMEM((2 * plan.q_end, D), BF16),
            pltpu.VMEM((length, plan.width), BF16),
            pltpu.VMEM((length, 2 * plan.q_end), BF16),
            pltpu.VMEM((length, D), BF16),
            pltpu.VMEM((halves * n_columns, plan.rows, share), BF16),
            sem,
            sem,
            pltpu.SemaphoreType.DMA((3,)),
            pltpu.SemaphoreType.DMA((halves * n_columns,)),
        ],
        compiler_params=PARAMS,
        name="probe",
    )(table, cosine, sine, fields, normed, mixed, w_out, *flat(p_pieces))
    curv_share = lax.dynamic_slice_in_dim(curvature[0], column * share, share, 1)
    weighted = []
    for j, (first, end) in enumerate(row_blocks(plan)):
        own, other = reduce_columns(tangents[j * n_columns : (j + 1) * n_columns], n_columns)
        if weighted:
            other = tie(other, mine)
        total = own.astype(F32) + other.astype(F32)
        mine = (curv_share[first:end].astype(F32) * total).astype(BF16)
        weighted += gather_columns(mine, n_columns)

    pieces = pl.pallas_call(
        lambda *refs: pull_kernel(plan, n_columns, *refs),
        out_shape=[
            jax.ShapeDtypeStruct((hi - lo, BLK, BLK), BF16)
            for _, lo, hi in plan.streams
            for _ in range(n)
        ],
        in_specs=[SMEM, HBM] + [VMEM] * (5 + halves * n_columns),
        out_specs=[ANY] * n_refs,
        scratch_shapes=[
            pltpu.VMEM((D, plan.width), BF16),
            pltpu.VMEM((plan.q_end, D), BF16),
            pltpu.VMEM((length, plan.q_end), BF16),
            pltpu.VMEM((length, plan.width), BF16),
            pltpu.VMEM((D, length), BF16),
            pltpu.VMEM((length, plan.kv_heads * HD), F32),
            pltpu.VMEM((length, plan.kv_heads * HD), F32),
            sem,
            sem,
            sem,
        ],
        compiler_params=PARAMS,
        name="pull",
    )(table, normed_t, w_out, fields, mixed_t, cosine, sine, *weighted)

    pieces = [pieces[k * n : (k + 1) * n] for k in range(len(plan.streams))]
    summed = reduce_ring(plan, pieces, 1.0 / jnp.sqrt(F32(length * n_owners)))
    live = jnp.arange(slots, dtype=jnp.int32) < counts[me]
    return jnp.where(live[:, None, None], summed, 0.0)[None]


def solution(mesh):
    in_specs = (
        P("fsdp", None, None),
        P(),
        P("fsdp", None, None),
        P("seq", "fsdp", None, None),
        P("seq", "fsdp", None, None),
        P("seq", None),
    )
    out_specs = P("seq", "fsdp", None, None)
    return jax.shard_map(local, mesh=mesh, in_specs=in_specs, out_specs=out_specs, check_vma=False)
```
